32 devices in a mesh: kgrp: 8 (over y, x, core), img: 4 (over z).
Axes of the slice: x: 2, y: 2, z: 4, core: 2. Of those that a mesh axis runs over, the one named last changes fastest.
Arguments:
- vectors: float32 [2, 16, 1024], P(None, 'img', 'kgrp'), may hold values from -6 to 6
- conduction: bfloat16 [16, 2, 8, 4, 4096], P('kgrp', None, None, 'img'), may hold values from -6 to 6
- valence: bfloat16 [16, 2, 8, 4, 4096], P('kgrp', None, None, 'img'), may hold values from -6 to 6
- hole_point: int32 [1], replicated, may hold values from 0 to 16383
- kpoint_grid: int32 [3, 16], replicated, may hold values from 0 to 11
- image_cells: int32 [3, 512], replicated, may hold values from -6 to 6
Outputs:
- psi_real: float32 [16, 4, 4096, 512], P(None, 'img', 'kgrp')
- psi_imag: float32 [16, 4, 4096, 512], P(None, 'img', 'kgrp')
The draws below stay inside these ranges and needn't reach their ends.
All inputs are finite; a program needn't handle non-finite values.
Results may differ from the reference program's by a relative error of at most 0.0043.
Values may be sent and summed in bfloat16 or wider, within the bound.
No kernel may reach another device: no remote copies, remote signals or barrier semaphores. Data moves between devices by JAX's collectives and lax.ppermute only.
A program may use at most 128 MiB of HBM per device.

```python
import jax
import jax.numpy as jnp
import numpy as np
from jax import lax

S = 16
NV = 8
NC = 8
NPTS = 16384
NR = 512
K = 16
NT = 1024
SLABS = 4
SLAB_PTS = 4096
N_KGRP = 8


def set_ends(values, rng, least, largest):
    spot = [jax.random.randint(jax.random.fold_in(rng, axis), (), 0, length) for axis, length in enumerate(values.shape)]
    longest = values.shape.index(max(values.shape))
    beside = spot[:longest] + [(spot[longest] + 1) % values.shape[longest]] + spot[longest + 1:]
    return values.at[tuple(spot)].set(least).at[tuple(beside)].set(largest)


def block_levels(stream_key, shape, split, low, high):
    def one(position, parts):
        draws = jax.random.uniform(jax.random.fold_in(jax.random.fold_in(stream_key, 6), position), (parts,), jnp.float32, low / len(split), high / len(split))
        return jnp.repeat(jnp.exp(draws), shape[position] // parts).reshape((-1,) + (1,) * (len(shape) - position - 1))

    factor_of = one(*split[0])
    for cut in split[1:]:
        factor_of = factor_of * one(*cut)
    return factor_of


def noise(key, shape, width, limit, split=(), held_as=jnp.bfloat16):
    values = width * jax.random.normal(key, shape, jnp.float32)
    if split:
        values = values * block_levels(key, shape, split, -0.22, 0.18)
    return jnp.clip(values, -limit, limit).astype(held_as)


def setup_inputs(seed: int = 0) -> dict:
    arg_keys = jax.random.split(jax.random.key(seed), 7)
    vectors = noise(arg_keys[0], (2, S, NT), 1.0, 6.0, ((1, 4), (2, 8)), jnp.float32)
    conduction = noise(arg_keys[1], (K, 2, NC, SLABS, SLAB_PTS), 1.0, 6.0, ((0, 8), (3, 4)))
    valence = noise(arg_keys[2], (K, 2, NV, SLABS, SLAB_PTS), 1.0, 6.0, ((0, 8), (3, 4)))
    hole_point = jax.random.randint(arg_keys[3], (1,), 0, NPTS).astype(jnp.int32)
    kpoint_grid = set_ends(jax.random.randint(arg_keys[4], (3, K), 0, 12), jax.random.fold_in(arg_keys[4], 1), 0, 11).astype(jnp.int32)
    image_cells = set_ends(jax.random.randint(arg_keys[5], (3, NR), -6, 7), jax.random.fold_in(arg_keys[5], 1), -6, 6).astype(jnp.int32)
    return {"vectors": vectors, "conduction": conduction, "valence": valence, "hole_point": hole_point, "kpoint_grid": kpoint_grid, "image_cells": image_cells}


cosine_levels = np.cos(2.0 * np.pi * np.arange(12) / 12.0)
sine_levels = np.sin(2.0 * np.pi * np.arange(12) / 12.0)


def phase_table(kpoint_grid, image_cells):
    turn_count = kpoint_grid[0][:, None] * image_cells[0][None, :]
    turn_count = turn_count + kpoint_grid[1][:, None] * image_cells[1][None, :]
    turn_count = turn_count + kpoint_grid[2][:, None] * image_cells[2][None, :]
    turn_count = jnp.mod(turn_count, 12)
    cosine = jnp.zeros(turn_count.shape, jnp.float32)
    sine_part = jnp.zeros(turn_count.shape, jnp.float32)
    for level_index in range(12):
        matches = turn_count == level_index
        cosine = jnp.where(matches, jnp.float32(cosine_levels[level_index]), cosine)
        sine_part = jnp.where(matches, jnp.float32(sine_levels[level_index]), sine_part)
    upper_half = jnp.stack([cosine, sine_part], 1)
    lower_half = jnp.stack([-sine_part, cosine], 1)
    return jnp.stack([upper_half, lower_half], 0).astype(jnp.bfloat16)


def hole_weights(amplitudes, hole_values):
    norm_factor = (NV * NC) ** -0.5
    real_amplitude = amplitudes[0]
    imaginary_amplitude = amplitudes[1]
    real_hole = hole_values[:, 0]
    imaginary_hole = hole_values[:, 1]
    highest = lax.Precision.HIGHEST
    weight_real = jnp.einsum("skvc,kv->ksc", real_amplitude, real_hole, precision=highest)
    weight_real = weight_real + jnp.einsum("skvc,kv->ksc", imaginary_amplitude, imaginary_hole, precision=highest)
    weight_imaginary = jnp.einsum("skvc,kv->ksc", imaginary_amplitude, real_hole, precision=highest)
    weight_imaginary = weight_imaginary - jnp.einsum("skvc,kv->ksc", real_amplitude, imaginary_hole, precision=highest)
    return jnp.stack([weight_real * norm_factor, weight_imaginary * norm_factor], 1).astype(jnp.bfloat16)


def mixing(weights):
    weight_real = weights[:, 0]
    weight_imaginary = weights[:, 1]
    first_row = jnp.stack([weight_real, -weight_imaginary], 2)
    second_row = jnp.stack([weight_imaginary, weight_real], 2)
    return jnp.stack([first_row, second_row], 1)


def reference(vectors, conduction, valence, hole_point, kpoint_grid, image_cells):
    group_size = N_KGRP
    blocks = NT // (group_size * group_size)
    ordered = vectors.reshape(2, S, group_size, group_size, blocks)
    ordered = ordered.transpose(0, 1, 3, 2, 4).reshape(2, S, K, NV, NC)
    flat_val = valence.reshape(K, 2, NV, NPTS)
    hole_values = lax.dynamic_slice_in_dim(flat_val, hole_point[0].astype(jnp.int32), 1, 3)[..., 0].astype(jnp.float32)
    weights = hole_weights(ordered, hole_values)
    coupling = mixing(weights).astype(jnp.float32)
    phases = phase_table(kpoint_grid, image_cells).astype(jnp.float32)
    flat_cond = conduction.reshape(K, 2, NC, NPTS)
    block_width = 512
    highest = lax.Precision.HIGHEST

    def one_block(offset):
        cond_block = lax.dynamic_slice_in_dim(flat_cond, offset, block_width, 3).astype(jnp.float32)
        products = jnp.einsum("kasbc,kbcp->sakp", coupling, cond_block, precision=highest).astype(jnp.bfloat16)
        products = lax.optimization_barrier(products).astype(jnp.float32)
        return jnp.einsum("sakp,akbn->spbn", products, phases, precision=highest)

    starts = (jnp.arange(NPTS // block_width) * block_width).astype(jnp.int32)
    summed = lax.map(one_block, starts)
    summed = summed.transpose(1, 0, 2, 3, 4).reshape(S, SLABS, SLAB_PTS, 2, NR) * (2 * K) ** -0.5
    return summed[:, :, :, 0, :], summed[:, :, :, 1, :]
```

```python
import functools

import jax
import jax.numpy as jnp
import numpy as np
from jax import lax
from jax.experimental import pallas as pl
from jax.experimental.pallas import tpu as pltpu
from jax.sharding import PartitionSpec as P


NV = 8
NC = 8
LANES = 128
MIB = 1 << 20

cosine_levels = np.cos(2.0 * np.pi * np.arange(12) / 12.0)
sine_levels = np.sin(2.0 * np.pi * np.arange(12) / 12.0)

VMEM = pltpu.MemorySpace.VMEM
SMEM = pltpu.MemorySpace.SMEM
ANY = pl.ANY


def iota(shape, axis):
    return lax.broadcasted_iota(jnp.int32, shape, axis)


def pack_kernel(slab_width, hole_ref, vector_ref, valence_ref, out_ref):
    local_k = valence_ref.shape[0]
    own = vector_ref.shape[1]
    width = vector_ref.shape[2]
    hole = hole_ref[0]
    present = hole // slab_width == lax.axis_index("img")
    lane = jnp.where(present, lax.rem(lax.rem(hole, slab_width), LANES), -1)
    keep = iota((NV, LANES), 1) == lane
    target = iota((NV, width), 1) // NC - iota((NV, width), 0)
    rows = []
    for part in range(2):
        spread = jnp.zeros((NV, width), jnp.float32)
        for q in range(local_k):
            values = jnp.where(keep, valence_ref[q, part].astype(jnp.float32), 0.0)
            column = jnp.sum(values, axis=1, keepdims=True)
            spread = jnp.where(target == q * NV, column, spread)
        rows.append(jnp.sum(spread, axis=0, keepdims=True))
    pad = out_ref.shape[1] - 2 * own - 2
    block = jnp.concatenate(
        [vector_ref[0], vector_ref[1]] + rows + [jnp.zeros((pad, width), jnp.float32)], 0
    )
    out_ref[...] = jnp.broadcast_to(block[None], out_ref.shape)


def pack(vectors, valence, hole_point, devices):
    own, width = vectors.shape[1:]
    slab_width = valence.shape[3]
    local_k = valence.shape[0]
    rows = -(-(2 * own + 2) // 8) * 8
    return pl.pallas_call(
        functools.partial(pack_kernel, slab_width),
        out_shape=jax.ShapeDtypeStruct((devices, rows, width), jnp.float32),
        grid_spec=pltpu.PrefetchScalarGridSpec(
            num_scalar_prefetch=1,
            grid=(1,),
            in_specs=[
                pl.BlockSpec((2, own, width), lambda i, h: (0, 0, 0)),
                pl.BlockSpec(
                    (local_k, 2, NV, LANES),
                    lambda i, h: (0, 0, 0, lax.rem(h[0], slab_width) // LANES),
                ),
            ],
            out_specs=pl.BlockSpec((devices, rows, width), lambda i, h: (0, 0, 0)),
        ),
        compiler_params=pltpu.CompilerParams(vmem_limit_bytes=4 * MIB),
        name="pack",
    )(hole_point, vectors, valence)


def cut_kernel(cond_ref, *outs):
    me = lax.axis_index("kgrp")
    width = outs[0].shape[-1]
    for step, out_ref in enumerate(outs):
        start = pl.multiple_of(jnp.bitwise_xor(me, step) * width, width)
        out_ref[...] = cond_ref[:, :, :, pl.ds(start, width)]


def cut(cond, group):
    piece = cond.shape[:3] + (cond.shape[3] // group,)
    return pl.pallas_call(
        cut_kernel,
        out_shape=[jax.ShapeDtypeStruct(piece, cond.dtype)] * group,
        in_specs=[pl.BlockSpec(memory_space=VMEM)],
        out_specs=[pl.BlockSpec(memory_space=VMEM)] * group,
        compiler_params=pltpu.CompilerParams(vmem_limit_bytes=4 * MIB),
        name="cut",
    )(cond)


def blocks_of(local_k, width):
    chunks = [(q, j) for q in range(local_k) for j in range(width // LANES)]
    return [chunks[i:i + 2] for i in range(0, len(chunks), 2)]


def stage_kernel(blocks, grid_ref, cells_ref, *refs):
    pieces, (points_ref, phase_ref, held) = refs[:-3], refs[-3:]
    me = lax.axis_index("kgrp")
    local_k = pieces[0].shape[0]
    for step, piece in enumerate(pieces):
        held[jnp.bitwise_xor(me, step)] = piece[...].reshape(held.shape[1:])
    images = cells_ref.shape[1]
    places = phase_ref.shape[1]
    for index, block in enumerate(blocks):
        parts = []
        owners = []
        for q, j in block:
            owners += [(8 * j + i) * local_k + q for i in range(8)]
            for i in range(8):
                parts.append(held[8 * j + i, q].astype(jnp.float32))
        points_ref[index] = jnp.concatenate(parts, 0).T.astype(jnp.bfloat16)
        row = iota((16, images), 0)
        turn = jnp.zeros((16, images), jnp.int32)
        for axis in range(3):
            column = jnp.zeros((16, images), jnp.int32)
            for place, k in enumerate(owners):
                column = jnp.where(row == place, grid_ref[axis, k], column)
            turn = turn + column * cells_ref[axis:axis + 1, :]
        count = turn.astype(jnp.float32)
        count = count - 12.0 * jnp.floor((count + 0.5) / 12.0)
        cosine = jnp.zeros((16, images), jnp.float32)
        sine = jnp.zeros((16, images), jnp.float32)
        for level in range(12):
            match = count == float(level)
            cosine = jnp.where(match, float(cosine_levels[level]), cosine)
            sine = jnp.where(match, float(sine_levels[level]), sine)
        upper = jnp.concatenate([cosine, sine], 1)
        lower = jnp.concatenate([-sine, cosine], 1)
        table = jnp.concatenate([upper, lower], 0).astype(jnp.bfloat16)
        phase_ref[index] = jnp.zeros(phase_ref.shape[1:], jnp.bfloat16)
        for place in range(places):
            phase_ref[index, place, 32 * place:32 * place + 32, :] = table


def stage(kpoint_grid, image_cells, pieces, width):
    group = len(pieces)
    local_k, _, _, points = pieces[0].shape
    images = image_cells.shape[1]
    blocks = blocks_of(local_k, width)
    return pl.pallas_call(
        functools.partial(stage_kernel, blocks),
        out_shape=[
            jax.ShapeDtypeStruct((len(blocks), points, 256), jnp.bfloat16),
            jax.ShapeDtypeStruct((len(blocks), 4, LANES, 2 * images), jnp.bfloat16),
        ],
        in_specs=[pl.BlockSpec(memory_space=SMEM)]
        + [pl.BlockSpec(memory_space=VMEM)] * (1 + group),
        out_specs=[pl.BlockSpec(memory_space=VMEM)] * 2,
        scratch_shapes=[pltpu.VMEM((group, local_k, 2 * NC, points), jnp.bfloat16)],
        compiler_params=pltpu.CompilerParams(vmem_limit_bytes=12 * MIB),
        name="stage",
    )(kpoint_grid, image_cells, *pieces)


def swap_blocks(x, block):
    count, width = x.shape
    row = iota(x.shape, 0)
    column = iota(x.shape, 1) // block
    step = 1
    while step < count:
        low_row = (row & step) == 0
        low_column = (column & step) == 0
        down = pltpu.roll(pltpu.roll(x, count - step, 0), step * block, 1)
        up = pltpu.roll(pltpu.roll(x, step, 0), width - step * block, 1)
        x = jnp.where(low_row == low_column, x, jnp.where(low_row, down, up))
        step *= 2
    return x


def psi_kernel(blocks, own, img, all_ref, points_ref, phase_ref, real_ref, imag_ref, table, product, out, sems):
    devices, _, width = all_ref.shape
    group = devices // img
    excitons = own * img
    block = width // group
    per_k = NV * NC // block
    points = points_ref.shape[1]
    images = phase_ref.shape[3] // 2
    norm_factor = (NV * NC) ** (-0.5)
    scale = (32 * len(blocks)) ** (-0.5)

    hole_real = []
    hole_imag = []
    for i in range(group):
        total = all_ref[i * img, 2 * own:, :]
        for z in range(1, img):
            total = total + all_ref[i * img + z, 2 * own:, :]
        hole_real.append(total[0:1])
        hole_imag.append(total[1:2])
    hole_real = swap_blocks(jnp.concatenate(hole_real, 0), block)
    hole_imag = swap_blocks(jnp.concatenate(hole_imag, 0), block)
    shape = (2 * own, width)
    sign = jnp.where(iota(shape, 0) < own, 1.0, -1.0)
    low = (iota(shape, 1) // NC) % 2 == 0
    coupled = {}
    for q in range(width // (NV * NC)):
        for z in range(img):
            total = jnp.zeros(shape, jnp.float32)
            for d in range(q * per_k, (q + 1) * per_k):
                x = all_ref[d * img + z, :2 * own, :]
                turned = pltpu.roll(x, own, 0)
                total = total + x * hole_real[d:d + 1] + sign * turned * hole_imag[d:d + 1]
            other = jnp.where(low, pltpu.roll(total, width - NC, 1), pltpu.roll(total, NC, 1))
            total = (total + other) * norm_factor
            total = jnp.where(low, total, -sign * pltpu.roll(total, own, 0))
            coupled[q, z] = total
    place = iota((16, LANES), 0)
    column = iota((16, LANES), 1) // (2 * NC)
    for index, pair in enumerate(blocks):
        for z in range(img):
            for e in range(own):
                s = z * own + e
                for part in range(2):
                    for half, (q, j) in enumerate(pair):
                        line = coupled[q, z][part * own + e:part * own + e + 1, j * LANES:(j + 1) * LANES]
                        spread = jnp.where(place == column + 8 * half, line, 0.0)
                        table[
                            index,
                            32 * s + 16 * part:32 * s + 16 * part + 16,
                            half * LANES:(half + 1) * LANES,
                        ] = spread.astype(jnp.bfloat16)
        for g in range(excitons // 4):
            product[index, g] = lax.dot_general(
                points_ref[index],
                table[index, g * LANES:(g + 1) * LANES, :],
                (((1,), (1,)), ((), ())),
                preferred_element_type=jnp.float32,
            ).astype(jnp.bfloat16)

    slots, _, rows, _ = out.shape
    cuts = points // rows
    steps = excitons * cuts

    def copies(step, slot):
        s = step // cuts
        start = lax.rem(step, cuts) * rows
        return [
            pltpu.make_async_copy(
                out.at[slot, part],
                ref.at[s, 0, pl.ds(start, rows), :],
                sems.at[slot, part],
            )
            for part, ref in enumerate((real_ref, imag_ref))
        ]

    @pl.loop(0, steps)
    def _(step):
        slot = lax.rem(step, slots)

        @pl.when(step >= slots)
        def _():
            for copy in copies(step - slots, slot):
                copy.wait()

        s = step // cuts
        start = pl.multiple_of(lax.rem(step, cuts) * rows, rows)
        for part in range(2):
            total = None
            for index in range(len(blocks)):
                term = jnp.dot(
                    product[index, s // 4, pl.ds(start, rows), :],
                    phase_ref[index, lax.rem(s, 4), :, part * images:(part + 1) * images],
                    preferred_element_type=jnp.float32,
                )
                total = term if total is None else total + term
            out[slot, part] = total * scale
        for copy in copies(step, slot):
            copy.start()

    for step in range(steps - slots, steps):
        for copy in copies(step, step % slots):
            copy.wait()


def psi(gathered, points, phases, own, img):
    width = gathered.shape[2]
    local_k = width // (NV * NC)
    blocks = blocks_of(local_k, width)
    excitons = own * img
    count = points.shape[1]
    images = phases.shape[3] // 2
    rows = min(count, 512)
    shape = jax.ShapeDtypeStruct((excitons, 1, count, images), jnp.float32)
    return pl.pallas_call(
        functools.partial(psi_kernel, blocks, own, img),
        out_shape=[shape, shape],
        in_specs=[pl.BlockSpec(memory_space=VMEM)] * 3,
        out_specs=[pl.BlockSpec(memory_space=ANY)] * 2,
        scratch_shapes=[
            pltpu.VMEM((len(blocks), 32 * excitons, 256), jnp.bfloat16),
            pltpu.VMEM((len(blocks), excitons // 4, count, LANES), jnp.bfloat16),
            pltpu.VMEM((4, 2, rows, images), jnp.float32),
            pltpu.SemaphoreType.DMA((4, 2)),
        ],
        compiler_params=pltpu.CompilerParams(vmem_limit_bytes=24 * MIB),
        name="psi",
    )(gathered, points, phases)


def phase_table(kpoint_grid, image_cells):
    turn_count = kpoint_grid[0][:, None] * image_cells[0][None, :]
    turn_count = turn_count + kpoint_grid[1][:, None] * image_cells[1][None, :]
    turn_count = turn_count + kpoint_grid[2][:, None] * image_cells[2][None, :]
    turn_count = jnp.mod(turn_count, 12)
    cosine = jnp.zeros(turn_count.shape, jnp.float32)
    sine_part = jnp.zeros(turn_count.shape, jnp.float32)
    for level_index in range(12):
        matches = turn_count == level_index
        cosine = jnp.where(matches, jnp.float32(cosine_levels[level_index]), cosine)
        sine_part = jnp.where(matches, jnp.float32(sine_levels[level_index]), sine_part)
    upper_half = jnp.stack([cosine, sine_part], 1)
    lower_half = jnp.stack([-sine_part, cosine], 1)
    return jnp.stack([upper_half, lower_half], 0).astype(jnp.bfloat16)


def hole_weights(amplitudes, hole_values):
    norm_factor = (NV * NC) ** (-0.5)
    real_amplitude = amplitudes[0]
    imaginary_amplitude = amplitudes[1]
    real_hole = hole_values[:, 0]
    imaginary_hole = hole_values[:, 1]
    highest = lax.Precision.HIGHEST
    weight_real = jnp.einsum("skvc,kv->ksc", real_amplitude, real_hole, precision=highest)
    weight_real = weight_real + jnp.einsum(
        "skvc,kv->ksc", imaginary_amplitude, imaginary_hole, precision=highest
    )
    weight_imaginary = jnp.einsum("skvc,kv->ksc", imaginary_amplitude, real_hole, precision=highest)
    weight_imaginary = weight_imaginary - jnp.einsum(
        "skvc,kv->ksc", real_amplitude, imaginary_hole, precision=highest
    )
    return jnp.stack([weight_real * norm_factor, weight_imaginary * norm_factor], 1).astype(
        jnp.bfloat16
    )


def mixing(weights):
    weight_real = weights[:, 0]
    weight_imaginary = weights[:, 1]
    first_row = jnp.stack([weight_real, -weight_imaginary], 2)
    second_row = jnp.stack([weight_imaginary, weight_real], 2)
    return jnp.stack([first_row, second_row], 1)


def general_shards(vectors, conduction, valence, hole_point, kpoint_grid, image_cells):
    group_size = lax.axis_size("kgrp")
    local_k = conduction.shape[0]
    slab_width = conduction.shape[4]
    own_excitons = vectors.shape[1]
    blocks = vectors.shape[2] // group_size
    columns = vectors.reshape(2, own_excitons, group_size, blocks)
    owned_columns = lax.all_to_all(columns, "kgrp", split_axis=2, concat_axis=2, tiled=True)
    owned_columns = owned_columns.reshape(2, own_excitons, local_k, NV, NC)
    hole_offset = hole_point[0] % slab_width
    hole_slab = hole_point[0] // slab_width
    present = (lax.axis_index("img") == hole_slab).astype(jnp.float32)
    picked = (
        lax.dynamic_slice_in_dim(valence[:, :, :, 0, :], hole_offset, 1, 3)[..., 0].astype(
            jnp.float32
        )
        * present
    )
    hole_values = lax.psum(picked, "img")
    weights = lax.all_gather(hole_weights(owned_columns, hole_values), "img", axis=2, tiled=True)
    phases = phase_table(kpoint_grid, image_cells)
    products = jnp.einsum(
        "kasbc,kbcp->sakp",
        mixing(weights),
        conduction[:, :, :, 0, :],
        preferred_element_type=jnp.float32,
    ).astype(jnp.bfloat16)
    summed = jnp.einsum(
        "sakp,akbn->spbn",
        lax.all_to_all(products, "kgrp", split_axis=3, concat_axis=2, tiled=True),
        phases,
        preferred_element_type=jnp.float32,
    )
    normal_scale = (2 * kpoint_grid.shape[1]) ** (-0.5)
    summed = summed * normal_scale
    return (summed[:, None, :, 0, :], summed[:, None, :, 1, :])


def shards(vectors, conduction, valence, hole_point, kpoint_grid, image_cells):
    group = lax.axis_size("kgrp")
    img = lax.axis_size("img")
    own = vectors.shape[1]
    width = vectors.shape[2]
    points = conduction.shape[4] // group
    if width // group != 2 * NC or width % LANES or points % LANES or group & (group - 1) or own != 4:
        return general_shards(vectors, conduction, valence, hole_point, kpoint_grid, image_cells)
    packed = pack(vectors, valence[:, :, :, 0, :], hole_point, group * img)
    gathered = lax.all_to_all(packed, ("kgrp", "img"), 0, 0, tiled=True)
    pieces = list(cut(conduction[:, :, :, 0, :], group))
    for step in range(1, group):
        pairs = [(i, i ^ step) for i in range(group)]
        pieces[step] = lax.ppermute(pieces[step], "kgrp", pairs)
    points, phases = stage(kpoint_grid, image_cells, pieces, width)
    real, imag = psi(gathered, points, phases, own, img)
    return real, imag


def solution(mesh):
    placed = (
        P(None, "img", "kgrp"),
        P("kgrp", None, None, "img", None),
        P("kgrp", None, None, "img", None),
        P(),
        P(),
        P(),
    )
    return jax.shard_map(
        shards,
        mesh=mesh,
        in_specs=placed,
        out_specs=(P(None, "img", "kgrp", None), P(None, "img", "kgrp", None)),
        check_vma=False,
    )
```
